32 devices in a mesh: plane: 4 (over y, x), tile: 8 (over z, core).
Axes of the slice: x: 2, y: 2, z: 4, core: 2. Of those that a mesh axis runs over, the one named last changes fastest.
Arguments:
- visibility: float32 [2, 65536], P(None, ('plane', 'tile')), may hold values from -6 to 6
- target: int32 [65536, 1], P(('plane', 'tile')), may hold values from 0 to 31; in each aligned block of 2048 rows (0 to 2047, 2048 to 4095, ...) at most 128 rows name the same one
- offset: int32 [65536], P(('plane', 'tile')), may hold values from 0 to 2097151
- taps: float32 [8], replicated, may hold values from 0.1 to 1
- w_plane: float32 [4], P('plane'), may hold values from -300 to 300
Outputs:
- dirty_image: float32 [4096, 4096], P('plane', 'tile')
The draws below stay inside these ranges and needn't reach their ends.
Inputs may be any that keep to these rules, and one draw needn't show every extreme that they name: `target`: among the rows of one device no value occurs more than 128 times, and some value occurs exactly 128 times.
All inputs are finite; a program needn't handle non-finite values.
Results may differ from the reference program's by a relative error of at most 0.0042.
Values sent between devices are 32-bit elements; how exact they have to be, the bound alone decides.
A program may use at most 128 MiB of HBM per device.

```python
import math
import jax
import jax.numpy as jnp
import numpy as np
from jax import lax

G = 4096
KS = 8
VIS_DEV = 2048
PLANES = 4
ROWS = 512
CAP = 128
VIS_ALL = 65536
N_PLANE = 4
N_TILE = 8


def plant(entries, key, smallest, largest):
    spot = [jax.random.randint(jax.random.fold_in(key, axis), (), 0, length) for axis, length in enumerate(entries.shape)]
    main_axis = entries.shape.index(max(entries.shape))
    neighbour = spot[:main_axis] + [(spot[main_axis] + 1) % entries.shape[main_axis]] + spot[main_axis + 1:]
    return entries.at[tuple(spot)].set(smallest).at[tuple(neighbour)].set(largest)


def shard_levels(own_key, shape, pieces, low, largest):
    level = 1.0
    for dim, parts in pieces:
        draws = jax.random.uniform(jax.random.fold_in(jax.random.fold_in(own_key, 6), dim), (parts,), jnp.float32, low / len(pieces), largest / len(pieces))
        level = level * jnp.repeat(jnp.exp(draws), shape[dim] // parts).reshape((-1,) + (1,) * (len(shape) - 1 - dim))
    return level


def deal_out(key, own, number, rows, count, top, reach, lean):
    sequence = jax.random.permutation(key, count)
    packed, common = load_shares(count, rows * top, reach, lean, True), load_shares(count, rows * top, reach, lean, False)
    places = jnp.arange(count)

    def named(sizes, rotation):
        used = int((sizes > 0).sum())
        fixed = max(1, used // 4)
        shifted = fixed + (places - fixed + rotation * (used - fixed)) % max(1, count - fixed)
        return jnp.zeros((count,), jnp.int32).at[sequence[jnp.where(places < fixed, places, shifted)]].set(jnp.asarray(sizes, jnp.int32))

    sizes = jnp.where(number % 4 == 0, named(packed, number // 4), named(common, number - number // 4 - 1))
    mixed = jax.random.permutation(jax.random.fold_in(own, 3), count)
    donor, receiver = mixed[0:count // 2 * 2:2], mixed[1:count // 2 * 2:2]
    slack = jnp.minimum(sizes[donor] - 1, reach - sizes[receiver]) // 2
    slack = jnp.where((donor == sequence[0]) | (receiver == sequence[0]) | (sizes[receiver] == 0), 0, jnp.maximum(slack, 0))
    shifted = jax.random.randint(jax.random.fold_in(own, 4), (count // 2,), 0, 1 << 20) % (slack + 1)
    sizes = sizes.at[donor].add(-shifted).at[receiver].add(shifted)
    members = jnp.searchsorted(jnp.cumsum(sizes), jnp.arange(rows * top), side="right").astype(jnp.int32)
    grid = members.reshape(top, rows).T
    grid = grid[jax.random.permutation(jax.random.fold_in(own, 1), rows)]
    rotation = jax.random.randint(jax.random.fold_in(own, 2), (rows, 1), 0, top)
    return jnp.take_along_axis(grid, (jnp.arange(top)[None, :] + rotation) % top, axis=1)


def load_shares(number_of, total, limit, skew, full):
    weights = [(1 << 20) // math.isqrt(grade ** skew) + 1 for grade in range(1, number_of + 1)]
    largest = limit if full else min(limit, max(-(-total // number_of), total * weights[0] // sum(weights)))
    least = 1 if total - largest >= number_of - 1 else 0
    holding, spare = [largest] + [least] * (number_of - 1), total - largest - least * (number_of - 1)
    while spare > 0:
        free = [i for i in range(1, number_of) if holding[i] < largest] or [i for i in range(1, number_of) if holding[i] < limit]
        pool, budget = sum([weights[i] for i in free]), spare
        for i in free:
            more = min(limit - holding[i], max(1, budget * weights[i] // pool), spare)
            holding[i] = holding[i] + more
            spare = spare - more
    return np.array(holding)


def gaussian(rng, shape, deviation, most, shards=(), kind=jnp.bfloat16):
    result = deviation * jax.random.normal(rng, shape, jnp.float32)
    if shards:
        result = result * shard_levels(rng, shape, shards, -0.22, 0.18)
    return jnp.clip(result, -most, most).astype(kind)


def setup_inputs(seed: int = 0) -> dict:
    keys = jax.random.split(jax.random.key(seed), 6)
    visibility = gaussian(keys[0], (2, VIS_ALL), 1.0, 6.0, ((1, 32),), jnp.float32)
    target_keys = jax.random.split(jax.random.fold_in(keys[1], 1), VIS_ALL // VIS_DEV)
    target_turns = jax.random.permutation(jax.random.fold_in(keys[1], 3), VIS_ALL // VIS_DEV)
    target = jax.vmap(lambda own, number: deal_out(jax.random.fold_in(keys[1], 2), own, number, VIS_DEV, N_PLANE * N_TILE, 1, CAP, 2))(target_keys, target_turns).reshape((VIS_ALL, 1))
    offset = plant(jax.random.randint(keys[2], (VIS_ALL,), 0, ROWS * G), jax.random.fold_in(keys[2], 1), 0, (ROWS * G) - 1).astype(jnp.int32)
    taps = jnp.clip(jnp.exp(jax.random.uniform(keys[3], (KS,), jnp.float32, math.log(0.1), math.log(1.0))), 0.1, 1.0)
    w_plane = jnp.clip(jax.random.uniform(keys[4], (PLANES,), jnp.float32, -300.0, 300.0) * shard_levels(keys[4], (PLANES,), ((0, 4),), -0.4, 0.0), -300.0, 300.0)
    return dict(visibility=visibility, target=target, offset=offset, taps=taps, w_plane=w_plane)


def direction(index, length):
    return ((index + length // 2) % length - length // 2).astype(jnp.float32) * (0.5 / length)

def reference(visibility, target, offset, taps, w_plane):
    destination = target[:, 0]
    plane_of = destination // N_TILE
    tile_of = destination % N_TILE
    grid_row = tile_of * (G // N_TILE) + offset // G
    grid_col = offset % G
    kernel_len = taps.shape[0]
    count = visibility.shape[1]
    weight_re = lax.optimization_barrier((taps[None, :] * visibility[0][:, None]).astype(jnp.bfloat16)).astype(jnp.float32)
    weight_im = lax.optimization_barrier((taps[None, :] * visibility[1][:, None]).astype(jnp.bfloat16)).astype(jnp.float32)
    taps_round = lax.optimization_barrier(taps.astype(jnp.bfloat16)).astype(jnp.float32)
    shifts = jnp.arange(kernel_len, dtype=jnp.int32)
    row_index = (grid_row[:, None] + shifts[None, :]) % G
    col_index = (grid_col[:, None] + shifts[None, :]) % G
    row_full = jnp.broadcast_to(row_index[:, :, None], (count, kernel_len, kernel_len))
    col_full = jnp.broadcast_to(col_index[:, None, :], (count, kernel_len, kernel_len))
    lines = jnp.arange(G, dtype=jnp.int32)
    cosines = direction(lines, G)
    n_minus = jnp.sqrt(1.0 - cosines[:, None] * cosines[:, None] - cosines[None, :] * cosines[None, :]) - 1.0
    image = jnp.zeros((G, G), jnp.float32)
    for plane in range(N_PLANE):
        mask = (plane_of == plane).astype(jnp.float32)
        value_re = (weight_re * mask[:, None])[:, :, None] * taps_round[None, None, :]
        value_im = (weight_im * mask[:, None])[:, :, None] * taps_round[None, None, :]
        grid_re = jnp.zeros((G, G), jnp.float32).at[row_full, col_full].add(value_re)
        grid_im = jnp.zeros((G, G), jnp.float32).at[row_full, col_full].add(value_im)
        transformed = jnp.fft.ifft2(grid_re + 1j * grid_im) * (G * G)
        phase = 2.0 * math.pi * w_plane[plane] * n_minus
        image = image + (jnp.cos(phase) * jnp.real(transformed) - jnp.sin(phase) * jnp.imag(transformed))
    return image * (1.0 / math.sqrt(VIS_ALL))
```

```python
import functools
import math

import jax
import jax.numpy as jnp
import numpy as np
from jax import lax
from jax.experimental import pallas as pl
from jax.experimental.pallas import tpu as pltpu
from jax.sharding import PartitionSpec as P

G = 4096
CHUNK = 256
BASE = 64


def fitted(function, terms):
    nodes = np.cos((np.arange(400) + 0.5) * np.pi / 400)
    square = 0.125 * (nodes + 1.0)
    table = np.polynomial.chebyshev.Chebyshev.fit(
        square, function(np.sqrt(square)), terms - 1, domain=[0.0, 0.25]
    )
    return [float(v) for v in table.convert(kind=np.polynomial.Polynomial).coef]


COS_COEF = fitted(lambda x: np.cos(2.0 * np.pi * x), 7)
SIN_COEF = fitted(lambda x: np.sin(2.0 * np.pi * x) / x, 6)


def horner(coefficients, x):
    total = coefficients[-1]
    for value in coefficients[-2::-1]:
        total = total * x + value
    return total


def turn(cycles):
    part = cycles - jnp.round(cycles)
    square = part * part
    return horner(COS_COEF, square), part * horner(SIN_COEF, square)


def grid_kernel(columns, count_ref, first_ref, vis_ref, out_ref, acc_ref, table_ref):
    tile, step = pl.program_id(0), pl.program_id(1)
    rows = acc_ref.shape[0]

    @pl.when(step == 0)
    def _():
        acc_ref[...] = jnp.zeros_like(acc_ref)

    @pl.when(step * CHUNK < count_ref[tile])
    def _():
        vis_re = vis_ref[0, 0:1, :]
        vis_im = vis_ref[0, 1:2, :]
        encoded = vis_ref[0, 2:3, :] - 1.0
        row = jnp.floor(encoded * (1.0 / G))
        column = encoded - row * G
        unit = column * (1.0 / G)
        place = lax.broadcasted_iota(jnp.int32, (BASE, CHUNK), 0).astype(jnp.float32)
        base_cos, base_sin = turn(place * unit)
        jump = lax.broadcasted_iota(jnp.int32, (8, CHUNK), 0) * BASE + first_ref[0]
        jump_cos, jump_sin = turn(jump.astype(jnp.float32) * unit)
        lead_re = vis_re * jump_cos - vis_im * jump_sin
        lead_im = vis_re * jump_sin + vis_im * jump_cos
        for block in range(columns // BASE):
            one_re = lead_re[block : block + 1]
            one_im = lead_im[block : block + 1]
            start = block * BASE
            table_ref[start : start + BASE] = (base_cos * one_re - base_sin * one_im).astype(
                jnp.bfloat16
            )
            table_ref[columns + start : columns + start + BASE] = (
                base_cos * one_im + base_sin * one_re
            ).astype(jnp.bfloat16)
        lines = lax.broadcasted_iota(jnp.int32, (rows, CHUNK), 0)
        onehot = jnp.where(lines == row.astype(jnp.int32), 1.0, 0.0).astype(jnp.bfloat16)
        acc_ref[...] += lax.dot_general(
            onehot, table_ref[...], (((1,), (1,)), ((), ())), preferred_element_type=jnp.float32
        )

    @pl.when(step == pl.num_programs(1) - 1)
    def _():
        out_ref[0, 0] = acc_ref[:, :columns].astype(out_ref.dtype)
        out_ref[0, 1] = acc_ref[:, columns:].astype(out_ref.dtype)


def image_kernel(
    tiles, weight_ref, w_ref, grid_ref, dft_ref, twist_ref, line_ref, side_ref, out_ref,
    half_ref, mixed_ref, full_ref,
):
    digit = pl.program_id(0)
    rows, columns = grid_ref.shape[2], grid_ref.shape[3]
    half = tiles // 2
    step = 32

    @pl.when(digit == 0)
    def _():
        @pl.loop(0, rows // step)
        def _(index):
            part = pl.ds(pl.multiple_of(index * step, step), step)
            for t in range(half):
                for c in range(2):
                    low = grid_ref[t, c, part, :].astype(jnp.float32)
                    high = grid_ref[t + half, c, part, :].astype(jnp.float32)
                    half_ref[0, t, c, part, :] = low + high
                    half_ref[1, t, c, part, :] = low - high

    parity = lax.rem(digit, 2)

    @pl.loop(0, rows // step)
    def _(index):
        at = pl.multiple_of(index * step, step)
        part = pl.ds(at, step)
        total_re = half_ref[parity, 0, 0, part, :]
        total_im = half_ref[parity, 0, 1, part, :]
        for t in range(1, half):
            cos_t = weight_ref[0, digit * half + t]
            sin_t = weight_ref[1, digit * half + t]
            value_re = half_ref[parity, t, 0, part, :]
            value_im = half_ref[parity, t, 1, part, :]
            total_re = total_re + (value_re * cos_t - value_im * sin_t)
            total_im = total_im + (value_re * sin_t + value_im * cos_t)
        twist_cos = twist_ref[0, part, 0:1]
        twist_sin = twist_ref[0, part, 1:2]
        mixed_ref[part, :] = (total_re * twist_cos - total_im * twist_sin).astype(jnp.bfloat16)
        mixed_ref[pl.ds(rows + at, step), :] = (
            total_re * twist_sin + total_im * twist_cos
        ).astype(jnp.bfloat16)

    full_ref[...] = jnp.dot(dft_ref[...], mixed_ref[...], preferred_element_type=jnp.float32)
    w = w_ref[0]

    @pl.loop(0, rows // step)
    def _(index):
        at = pl.multiple_of(index * step, step)
        part = pl.ds(at, step)
        flat = line_ref[0, part, 0:1]
        line_angle = line_ref[0, part, 1:2]
        line_size = line_ref[0, part, 2:3]
        root = jnp.sqrt(flat - side_ref[0:1, :])
        cycles = w * (root - 1.0) + (line_angle + side_ref[1:2, :])
        cos_s, sin_s = turn(cycles)
        picture = cos_s * full_ref[part, :] - sin_s * full_ref[pl.ds(rows + at, step), :]
        out_ref[part, digit, :] = picture * (
            line_size * side_ref[2:3, :]
        )


def direction(index, length):
    return ((index + length // 2) % length - length // 2).astype(jnp.float32) * (0.5 / length)


def response(taps, index):
    shifts = jnp.arange(taps.shape[0], dtype=jnp.int32)
    angles = (shifts[None, :] * index[:, None] % G).astype(jnp.float32) * (2.0 * math.pi / G)
    real = jnp.sum(jnp.cos(angles) * taps[None, :], axis=1)
    imag = jnp.sum(jnp.sin(angles) * taps[None, :], axis=1)
    return jnp.arctan2(imag, real) * (0.5 / math.pi), jnp.sqrt(real * real + imag * imag)


def local(visibility, target, offset, taps, w_plane):
    tiles = lax.axis_size("tile")
    planes = lax.axis_size("plane")
    devices = tiles * planes
    vis_dev = visibility.shape[1]
    capacity = 2 * vis_dev // devices
    slot_total = devices * capacity
    band = G // tiles
    columns = G // tiles
    destination = target[:, 0]
    onehot = (destination[:, None] == jnp.arange(devices, dtype=jnp.int32)[None, :]).astype(
        jnp.int32
    )
    rank = jnp.sum(jnp.cumsum(onehot, axis=0) * onehot, axis=1) - 1
    slot = destination * capacity + rank
    payload = jnp.stack([visibility[0], visibility[1], offset.astype(jnp.float32) + 1.0])
    outgoing = jnp.zeros((3, slot_total), jnp.float32).at[:, slot].set(payload)
    received = lax.all_to_all(outgoing, ("plane", "tile"), split_axis=1, concat_axis=1, tiled=True)
    used = received[2] > 0.0
    place = jnp.where(used, jnp.cumsum(used.astype(jnp.int32)) - 1, slot_total)
    packed = jnp.zeros((3, slot_total), jnp.float32).at[:, place].set(received, mode="drop")
    gathered = lax.all_gather(packed, "tile", axis=0)
    counts = jnp.sum((gathered[:, 2] > 0.0).astype(jnp.int32), axis=1)
    first = (lax.axis_index("tile") * columns).astype(jnp.int32)
    smem = pl.BlockSpec(memory_space=pltpu.SMEM)
    steps = slot_total // CHUNK
    grids = pl.pallas_call(
        functools.partial(grid_kernel, columns),
        grid=(tiles, steps),
        out_shape=jax.ShapeDtypeStruct((tiles, 2, band, columns), jnp.bfloat16),
        in_specs=[smem, smem, pl.BlockSpec((1, 3, CHUNK), lambda t, k: (t, 0, k))],
        out_specs=pl.BlockSpec((1, 2, band, columns), lambda t, k: (t, 0, 0, 0)),
        scratch_shapes=[
            pltpu.VMEM((band, 2 * columns), jnp.float32),
            pltpu.VMEM((2 * columns, CHUNK), jnp.bfloat16),
        ],
    )(counts, first[None], gathered)

    numbers = np.arange(band)
    angles = 2.0 * np.pi * (numbers[:, None] * numbers[None, :] % band) / band
    cos_d, sin_d = np.cos(angles), np.sin(angles)
    dft = np.block([[cos_d, -sin_d], [sin_d, cos_d]]).astype(jnp.bfloat16)
    digits = np.arange(tiles)
    angles = 2.0 * np.pi * (digits[:, None] * np.arange(tiles // 2)[None, :] % tiles) / tiles
    weights = np.stack([np.cos(angles).ravel(), np.sin(angles).ravel()]).astype(np.float32)
    angles = 2.0 * np.pi * (digits[:, None] * numbers[None, :]) / G
    twist = np.stack([np.cos(angles), np.sin(angles)], axis=2).astype(np.float32)

    line_pos = jnp.arange(G, dtype=jnp.int32)
    line_angle, line_size = response(taps, line_pos)
    cos_row = direction(line_pos, G)
    line = jnp.stack(
        [1.0 - cos_row * cos_row, line_angle, line_size * (1.0 / math.sqrt(vis_dev * devices))],
        axis=1,
    )
    line = line.reshape(band, tiles, 3).transpose(1, 0, 2)
    column_pos = first + jnp.arange(columns, dtype=jnp.int32)
    side_angle, side_size = response(taps.astype(jnp.bfloat16).astype(jnp.float32), column_pos)
    cos_col = direction(column_pos, G)
    side = jnp.stack([cos_col * cos_col, side_angle, side_size])

    screened = pl.pallas_call(
        functools.partial(image_kernel, tiles),
        grid=(tiles,),
        out_shape=jax.ShapeDtypeStruct((band, tiles, columns), jnp.float32),
        in_specs=[
            smem,
            smem,
            pl.BlockSpec((tiles, 2, band, columns), lambda d: (0, 0, 0, 0)),
            pl.BlockSpec((2 * band, 2 * band), lambda d: (0, 0)),
            pl.BlockSpec((1, band, 2), lambda d: (d, 0, 0)),
            pl.BlockSpec((1, band, 3), lambda d: (d, 0, 0)),
            pl.BlockSpec((3, columns), lambda d: (0, 0)),
        ],
        out_specs=pl.BlockSpec((band, tiles, columns), lambda d: (0, 0, 0)),
        scratch_shapes=[
            pltpu.VMEM((2, tiles // 2, 2, band, columns), jnp.float32),
            pltpu.VMEM((2 * band, columns), jnp.bfloat16),
            pltpu.VMEM((2 * band, columns), jnp.float32),
        ],
        compiler_params=pltpu.CompilerParams(vmem_limit_bytes=64 * 1024 * 1024 - 65536),
    )(jnp.asarray(weights), w_plane, grids, jnp.asarray(dft), jnp.asarray(twist), line, side)
    return lax.psum_scatter(screened.reshape(G, columns), "plane", scatter_dimension=0, tiled=True)


def solution(mesh):
    return jax.shard_map(
        local,
        mesh=mesh,
        in_specs=(
            P(None, ("plane", "tile")),
            P(("plane", "tile"), None),
            P(("plane", "tile")),
            P(),
            P("plane"),
        ),
        out_specs=P("plane", "tile"),
        check_vma=False,
    )
```
